512 devices in a mesh: dp: 32 (over y, x, core), tensor: 16 (over z).
Axes of the slice: x: 4, y: 4, z: 16, core: 2. Of those that a mesh axis runs over, the one named last changes fastest.
Arguments:
- tokens: bfloat16 [16384, 8192], P('dp', 'tensor'), may hold values from -6 to 6
- out_grad: bfloat16 [16384, 28672], P('dp', 'tensor'), may hold values from -6 to 6
- galore_basis: bfloat16 [8192, 512], P('tensor'), may hold values from -0.0625 to 0.0625
- first_moment: float32 [512, 28672], P('dp', 'tensor'), may hold values from -4 to 4
- second_moment: float32 [512, 28672], P('dp', 'tensor'), may hold values from 0.05 to 5
- list_lengths: int32 [128], P('dp'), may hold values from 1 to 128, as said below
Outputs:
- new_first: float32 [512, 28672], P('dp', 'tensor')
- new_second: float32 [512, 28672], P('dp', 'tensor')
- weight_step: bfloat16 [8192, 28672], P('dp', 'tensor')
The draws below stay inside these ranges and needn't reach their ends.
Inputs may be any that keep to these rules, and one draw needn't show every extreme that they name: `list_lengths`: live slots of a list come first in its 128 slots.
All inputs are finite; a program needn't handle non-finite values.
Results may differ from the reference program's by a relative error of at most 0.0051.
Values may be sent and summed in bfloat16 or wider, within the bound.
No kernel may reach another device: no remote copies, remote signals or barrier semaphores. Data moves between devices by JAX's collectives and lax.ppermute only.
A program may use at most 64 MiB of HBM per device.

```python
import math
import jax
import jax.numpy as jnp

D = 8192
FF = 28672
RANK = 512
SLOTS = 128
STEP = 1000
LISTS = 4
TOKENS = 16384
LISTS_ALL = 128
N_DP = 32


def draw_list_lengths(key, part):
    position = jnp.arange(LISTS_ALL, dtype=jnp.int32)
    replica = position // LISTS
    highest = SLOTS // 3 + (SLOTS - SLOTS // 3) * replica // (N_DP - 1)
    lowest = jnp.maximum(1, highest // 2)
    drawn = jax.random.randint(key, (LISTS_ALL,), lowest, highest + 1)
    drawn = jnp.where(position == 0, 1, drawn)
    return jnp.where(position == (N_DP - 1) * LISTS, SLOTS, drawn).astype(jnp.int32)


def level_of(own_key, dims, pieces, least, largest):
    loudness = 1.0
    for dim, shards_of in pieces:
        heights = jax.random.uniform(jax.random.fold_in(jax.random.fold_in(own_key, 6), dim), (shards_of,), jnp.float32, least / len(pieces), largest / len(pieces))
        loudness = loudness * jnp.repeat(jnp.exp(heights), dims[dim] // shards_of).reshape((-1,) + (1,) * (len(dims) - 1 - dim))
    return loudness


def bell_draw(stream_key, shape, scale, limit, shards=(), kind=jnp.bfloat16):
    level = level_of(stream_key, shape, shards, -0.22, 0.18) if shards else 1.0
    values = jax.random.normal(stream_key, shape, jnp.float32) * scale * level
    return jnp.minimum(jnp.maximum(values, -limit), limit).astype(kind)


def setup_inputs(seed: int = 0) -> dict:
    splits = jax.random.split(jax.random.key(seed), 7)
    tokens = bell_draw(splits[0], (TOKENS, D), 1.0, 6.0, ((0, 32), (1, 16)))
    out_grad = bell_draw(splits[1], (TOKENS, FF), 1.0, 6.0, ((0, 32), (1, 16)))
    galore_basis = bell_draw(splits[2], (D, RANK), D ** -0.5, 0.0625, ((0, 16),))
    first_moment = bell_draw(splits[3], (RANK, FF), 0.5, 4.0, ((0, 32), (1, 16)), jnp.float32)
    second_moment = jnp.clip(jnp.exp(math.log(5.0) - 4.6051702 * jax.random.uniform(splits[4], (RANK, FF), jnp.float32) ** level_of(splits[4], (RANK, FF), ((0, 32), (1, 16)), -0.2, 0.2)), 0.05, 5.0)
    list_lengths = draw_list_lengths(jax.random.fold_in(splits[6], 71), 0)
    return dict(tokens=tokens, out_grad=out_grad, galore_basis=galore_basis, first_moment=first_moment, second_moment=second_moment, list_lengths=list_lengths)


beta_first = 0.9
beta_second = 0.999
epsilon = 1e-08

def token_weights(list_lengths):
    slot_index = jnp.arange(SLOTS, dtype=jnp.int32)
    lengths = list_lengths.astype(jnp.int32)
    live_slots = slot_index[None, :] < lengths[:, None]
    scaled = jnp.where(live_slots, 1.0 / lengths[:, None].astype(jnp.float32), jnp.float32(0.0))
    return scaled.reshape(-1).astype(jnp.float32)

def reference(tokens, out_grad, galore_basis, first_moment, second_moment, list_lengths):
    coordinates = jnp.dot(tokens, galore_basis, preferred_element_type=jnp.float32)
    weighted = (coordinates * token_weights(list_lengths)[:, None]).astype(jnp.bfloat16)
    gradient = jnp.dot(weighted.T, out_grad, preferred_element_type=jnp.float32)
    new_first = beta_first * first_moment + (1.0 - beta_first) * gradient
    new_second = beta_second * second_moment + (1.0 - beta_second) * gradient * gradient
    corrected_first = new_first / (1.0 - beta_first ** STEP)
    corrected_second = new_second / (1.0 - beta_second ** STEP)
    update = (corrected_first / (jnp.sqrt(corrected_second) + epsilon)).astype(jnp.bfloat16)
    weight_step = (-jnp.dot(galore_basis, update, preferred_element_type=jnp.float32)).astype(jnp.bfloat16)
    return (new_first, new_second, weight_step)
```

```python
import jax
import jax.numpy as jnp
from jax import lax
from jax.sharding import PartitionSpec as P

SLOTS = 128
STEP = 1000


beta_first = 0.9
beta_second = 0.999
epsilon = 1e-08

bf16 = jnp.bfloat16
f32 = jnp.float32


def exchange(tiles, axis, groups=None):
    return lax.all_to_all(tiles, axis, split_axis=0, concat_axis=0, tiled=True, axis_index_groups=groups)


def copies_to_all(x, axis, peers, groups=None):
    return exchange(jnp.broadcast_to(x, (peers, *x.shape)), axis, groups)


def token_weights(list_lengths):
    slot_index = jnp.arange(SLOTS, dtype=jnp.int32)
    live_slots = slot_index[None, :] < list_lengths[:, None]
    scaled = jnp.where(
        live_slots, 1.0 / list_lengths[:, None].astype(jnp.float32), jnp.float32(0.0)
    )
    return scaled.reshape(-1)


def basis_routes(chips, splits):
    return [
        ((2 * k + b) * splits + s, (2 * s + b) * splits + (k - s) % splits)
        for k in range(chips)
        for b in range(2)
        for s in range(splits)
    ]


def body(tokens, out_grad, galore_basis, first_moment, second_moment, list_lengths):
    replicas = lax.axis_size("dp")
    splits = lax.axis_size("tensor")
    chips = replicas // 2
    replica = lax.axis_index("dp")
    core = replica % 2
    rank = galore_basis.shape[1]
    owned = rank // replicas
    columns = out_grad.shape[1]
    slots = tokens.shape[0]
    same_core = [[2 * i + c for i in range(chips)] for c in range(2)]
    partner = [(i, i ^ 1) for i in range(replicas)]

    block_rows = galore_basis.shape[0] * splits // replicas
    half_block = lax.dynamic_slice_in_dim(galore_basis, core * block_rows, block_rows, 0)
    local_basis = lax.ppermute(half_block, ("dp", "tensor"), basis_routes(chips, splits))

    partial = lax.dot_general(
        galore_basis, tokens, (((0,), (1,)), ((), ())), preferred_element_type=f32
    ).astype(bf16)
    arrived = exchange(partial.reshape(splits, rank // splits, slots), "tensor")
    coordinates = arrived.astype(f32).sum(axis=0)
    weighted = (coordinates * token_weights(list_lengths)[None, :]).astype(bf16)
    weighted = lax.all_gather(weighted, "tensor", axis=0, tiled=True)
    by_owner = weighted.reshape(chips, 2, owned, slots)
    other = lax.dynamic_index_in_dim(by_owner, 1 - core, 1, keepdims=False).reshape(rank // 2, slots)
    own = lax.dynamic_index_in_dim(by_owner, core, 1, keepdims=False).reshape(rank // 2, slots)
    sent = jnp.dot(other, out_grad, preferred_element_type=f32).astype(bf16)
    received = lax.ppermute(sent, "dp", partner)
    kept = jnp.dot(own, out_grad, preferred_element_type=f32)
    chip_sum = (kept + received.astype(f32)).astype(bf16).reshape(chips, owned, columns)
    gradient = exchange(chip_sum, "dp", same_core).astype(f32).sum(axis=0)

    new_first = beta_first * first_moment + (1.0 - beta_first) * gradient
    new_second = beta_second * second_moment + (1.0 - beta_second) * gradient * gradient
    corrected_first = new_first / (1.0 - beta_first**STEP)
    corrected_second = new_second / (1.0 - beta_second**STEP)
    update = (corrected_first / (jnp.sqrt(corrected_second) + epsilon)).astype(bf16)

    own_rows = copies_to_all(update, "dp", chips, same_core).reshape(rank // 2, columns)
    other_rows = lax.ppermute(own_rows, "dp", partner)
    place = jnp.arange(rank, dtype=jnp.int32)
    side = place // (rank // 2)
    within = place % (rank // 2)
    source = (within // owned) * (2 * owned) + jnp.where(side == 0, core, 1 - core) * owned + within % owned
    pick = (place[:, None] == source[None, :]).astype(bf16)
    ordered = jnp.dot(local_basis, pick, preferred_element_type=f32).astype(bf16)
    expanded = jnp.dot(ordered[:, : rank // 2], own_rows, preferred_element_type=f32)
    expanded = expanded + jnp.dot(ordered[:, rank // 2 :], other_rows, preferred_element_type=f32)
    weight_step = (-expanded).astype(bf16)
    return (new_first, new_second, weight_step)


def solution(mesh):
    in_specs = (
        P("dp", "tensor"),
        P("dp", "tensor"),
        P("tensor", None),
        P("dp", "tensor"),
        P("dp", "tensor"),
        P("dp"),
    )
    out_specs = (P("dp", "tensor"), P("dp", "tensor"), P("dp", "tensor"))
    return jax.shard_map(body, mesh=mesh, in_specs=in_specs, out_specs=out_specs, check_vma=False)
```

```python
import jax
import jax.numpy as jnp
from jax import lax
from jax.sharding import PartitionSpec as P


SLOTS = 128
STEP = 1000


beta_first = 0.9
beta_second = 0.999
epsilon = 1e-08

bf16 = jnp.bfloat16
f32 = jnp.float32


def exchange(tiles, axis, groups=None):
    return lax.all_to_all(tiles, axis, split_axis=0, concat_axis=0, tiled=True, axis_index_groups=groups)


def copies_to_all(x, axis, peers, groups=None):
    return exchange(jnp.broadcast_to(x, (peers, *x.shape)), axis, groups)


def token_weights(list_lengths):
    slot_index = jnp.arange(SLOTS, dtype=jnp.int32)
    live_slots = slot_index[None, :] < list_lengths[:, None]
    scaled = jnp.where(
        live_slots, 1.0 / list_lengths[:, None].astype(jnp.float32), jnp.float32(0.0)
    )
    return scaled.reshape(-1)


def basis_routes(chips, splits):
    return [
        ((2 * k + b) * splits + s, (2 * s + b) * splits + (k - s) % splits)
        for k in range(chips)
        for b in range(2)
        for s in range(splits)
    ]


def body(tokens, out_grad, galore_basis, first_moment, second_moment, list_lengths):
    replicas = lax.axis_size("dp")
    splits = lax.axis_size("tensor")
    chips = replicas // 2
    core = lax.axis_index("dp") % 2
    parity = lax.axis_index("tensor") % 2
    rank = galore_basis.shape[1]
    half = rank // 2
    owned = rank // replicas
    columns = out_grad.shape[1]
    slots = tokens.shape[0]
    same_core = [[2 * i + c for i in range(chips)] for c in range(2)]
    same_parity = [[2 * i + p for i in range(splits // 2)] for p in range(2)]
    other_core = [(i, i ^ 1) for i in range(replicas)]
    neighbor = [(i, i ^ 1) for i in range(splits)]

    def coordinates_of(side):
        part = lax.dynamic_slice_in_dim(galore_basis, side * half, half, 1)
        return lax.dot_general(part, tokens, (((0,), (1,)), ((), ())), preferred_element_type=f32)

    received = lax.ppermute(coordinates_of(1 - parity).astype(bf16), "tensor", neighbor)
    block_rows = galore_basis.shape[0] * splits // replicas
    half_block = lax.dynamic_slice_in_dim(galore_basis, core * block_rows, block_rows, 0)
    local_basis = lax.ppermute(half_block, ("dp", "tensor"), basis_routes(chips, splits))
    pair_sum = (coordinates_of(parity) + received.astype(f32)).astype(bf16)
    arrived = exchange(pair_sum.reshape(splits // 2, rank // splits, slots), "tensor", same_parity)
    coordinates = arrived.astype(f32).sum(axis=0)
    weighted = (coordinates * token_weights(list_lengths)[None, :]).astype(bf16)
    near = copies_to_all(weighted, "tensor", splits // 2, same_parity).reshape(half, slots)
    far = lax.ppermute(near, "tensor", neighbor)

    low = jnp.where(parity == 0, near, far).reshape(chips // 2, 2, owned, slots)
    high = jnp.where(parity == 0, far, near).reshape(chips // 2, 2, owned, slots)

    def rows_of(side):
        parts = [lax.dynamic_index_in_dim(x, side, 1, keepdims=False) for x in (low, high)]
        return jnp.concatenate(parts, axis=0).reshape(half, slots)

    sent = jnp.dot(rows_of(1 - core), out_grad, preferred_element_type=f32).astype(bf16)
    received = lax.ppermute(sent, "dp", other_core)
    kept = jnp.dot(rows_of(core), out_grad, preferred_element_type=f32)
    chip_sum = (kept + received.astype(f32)).astype(bf16).reshape(chips, owned, columns)
    gradient = exchange(chip_sum, "dp", same_core).astype(f32).sum(axis=0)

    new_first = beta_first * first_moment + (1.0 - beta_first) * gradient
    new_second = beta_second * second_moment + (1.0 - beta_second) * gradient * gradient
    corrected_first = new_first / (1.0 - beta_first**STEP)
    corrected_second = new_second / (1.0 - beta_second**STEP)
    update = (corrected_first / (jnp.sqrt(corrected_second) + epsilon)).astype(bf16)

    own_rows = copies_to_all(update, "dp", chips, same_core).reshape(half, columns)
    other_rows = lax.ppermute(own_rows, "dp", other_core)
    place = jnp.arange(rank, dtype=jnp.int32)
    within = place % half
    source = (within // owned) * (2 * owned) + jnp.where(place < half, core, 1 - core) * owned + within % owned
    pick = (place[:, None] == source[None, :]).astype(bf16)
    ordered = jnp.dot(local_basis, pick, preferred_element_type=f32).astype(bf16)
    expanded = jnp.dot(ordered[:, :half], own_rows, preferred_element_type=f32)
    expanded = expanded + jnp.dot(ordered[:, half:], other_rows, preferred_element_type=f32)
    weight_step = (-expanded).astype(bf16)
    return (new_first, new_second, weight_step)


def solution(mesh):
    in_specs = (
        P("dp", "tensor"),
        P("dp", "tensor"),
        P("tensor", None),
        P("dp", "tensor"),
        P("dp", "tensor"),
        P("dp"),
    )
    out_specs = (P("dp", "tensor"), P("dp", "tensor"), P("dp", "tensor"))
    return jax.shard_map(body, mesh=mesh, in_specs=in_specs, out_specs=out_specs, check_vma=False)
```

```python
import jax
import jax.numpy as jnp
from jax import lax
from jax.sharding import PartitionSpec as P


SLOTS = 128
STEP = 1000


beta_first = 0.9
beta_second = 0.999
epsilon = 1e-08

bf16 = jnp.bfloat16
f32 = jnp.float32


def exchange(tiles, axis, groups=None):
    return lax.all_to_all(tiles, axis, split_axis=0, concat_axis=0, tiled=True, axis_index_groups=groups)


def copies_to_all(x, axis, peers, groups=None):
    return exchange(jnp.broadcast_to(x, (peers, *x.shape)), axis, groups)


def token_weights(list_lengths):
    slot_index = jnp.arange(SLOTS, dtype=jnp.int32)
    live_slots = slot_index[None, :] < list_lengths[:, None]
    scaled = jnp.where(
        live_slots, 1.0 / list_lengths[:, None].astype(jnp.float32), jnp.float32(0.0)
    )
    return scaled.reshape(-1)


def basis_routes(chips, splits):
    return [
        ((2 * k + b) * splits + s, (2 * s + b) * splits + (k - s) % splits)
        for k in range(chips)
        for b in range(2)
        for s in range(splits)
    ]


def body(tokens, out_grad, galore_basis, first_moment, second_moment, list_lengths):
    replicas = lax.axis_size("dp")
    splits = lax.axis_size("tensor")
    chips = replicas // 2
    core = lax.axis_index("dp") % 2
    parity = lax.axis_index("tensor") % 2
    rank = galore_basis.shape[1]
    half = rank // 2
    owned = rank // replicas
    columns = out_grad.shape[1]
    slots = tokens.shape[0]
    same_core = [[2 * i + c for i in range(chips)] for c in range(2)]
    same_parity = [[2 * i + p for i in range(splits // 2)] for p in range(2)]
    other_core = [(i, i ^ 1) for i in range(replicas)]
    neighbor = [(i, i ^ 1) for i in range(splits)]

    def coordinates_of(side):
        part = lax.dynamic_slice_in_dim(galore_basis, side * half, half, 1)
        return lax.dot_general(part, tokens, (((0,), (1,)), ((), ())), preferred_element_type=f32)

    received = lax.ppermute(coordinates_of(1 - parity).astype(bf16), "tensor", neighbor)
    block_rows = galore_basis.shape[0] * splits // replicas
    half_block = lax.dynamic_slice_in_dim(galore_basis, core * block_rows, block_rows, 0)
    local_basis = lax.ppermute(half_block, ("dp", "tensor"), basis_routes(chips, splits))
    kept = lax.optimization_barrier(coordinates_of(parity))
    pair_sum = (kept + received.astype(f32)).astype(bf16)
    arrived = exchange(pair_sum.reshape(splits // 2, rank // splits, slots), "tensor", same_parity)
    coordinates = arrived.astype(f32).sum(axis=0)
    weighted = (coordinates * token_weights(list_lengths)[None, :]).astype(bf16)
    near = copies_to_all(weighted, "tensor", splits // 2, same_parity).reshape(half, slots)
    far = lax.ppermute(near, "tensor", neighbor)

    low = jnp.where(parity == 0, near, far).reshape(chips // 2, 2, owned, slots)
    high = jnp.where(parity == 0, far, near).reshape(chips // 2, 2, owned, slots)

    def rows_of(side):
        parts = [lax.dynamic_index_in_dim(x, side, 1, keepdims=False) for x in (low, high)]
        return jnp.concatenate(parts, axis=0).reshape(half, slots)

    sent = jnp.dot(rows_of(1 - core), out_grad, preferred_element_type=f32).astype(bf16)
    received = lax.ppermute(sent, "dp", other_core)
    kept = lax.optimization_barrier(jnp.dot(rows_of(core), out_grad, preferred_element_type=f32))
    chip_sum = (kept + received.astype(f32)).astype(bf16).reshape(chips, owned, columns)
    gradient = exchange(chip_sum, "dp", same_core).astype(f32).sum(axis=0)

    new_first = beta_first * first_moment + (1.0 - beta_first) * gradient
    new_second = beta_second * second_moment + (1.0 - beta_second) * gradient * gradient
    corrected_first = new_first / (1.0 - beta_first**STEP)
    corrected_second = new_second / (1.0 - beta_second**STEP)
    update = (corrected_first / (jnp.sqrt(corrected_second) + epsilon)).astype(bf16)

    own_rows = copies_to_all(update, "dp", chips, same_core).reshape(half, columns)
    other_rows = lax.ppermute(own_rows, "dp", other_core)
    place = jnp.arange(rank, dtype=jnp.int32)
    within = place % half
    source = (within // owned) * (2 * owned) + jnp.where(place < half, core, 1 - core) * owned + within % owned
    pick = (place[:, None] == source[None, :]).astype(bf16)
    ordered = jnp.dot(local_basis, pick, preferred_element_type=f32).astype(bf16)
    expanded = jnp.dot(ordered[:, :half], own_rows, preferred_element_type=f32)
    expanded = expanded + jnp.dot(ordered[:, half:], other_rows, preferred_element_type=f32)
    weight_step = (-expanded).astype(bf16)
    return (new_first, new_second, weight_step)


def solution(mesh):
    in_specs = (
        P("dp", "tensor"),
        P("dp", "tensor"),
        P("tensor", None),
        P("dp", "tensor"),
        P("dp", "tensor"),
        P("dp"),
    )
    out_specs = (P("dp", "tensor"), P("dp", "tensor"), P("dp", "tensor"))
    return jax.shard_map(body, mesh=mesh, in_specs=in_specs, out_specs=out_specs, check_vma=False)
```

```python
import jax
import jax.numpy as jnp
from jax import lax
from jax.sharding import PartitionSpec as P


SLOTS = 128
STEP = 1000


beta_first = 0.9
beta_second = 0.999
epsilon = 1e-08

bf16 = jnp.bfloat16
f32 = jnp.float32


def exchange(tiles, axis, groups=None):
    return lax.all_to_all(tiles, axis, split_axis=0, concat_axis=0, tiled=True, axis_index_groups=groups)


def copies_to_all(x, axis, peers, groups=None):
    return exchange(jnp.broadcast_to(x, (peers, *x.shape)), axis, groups)


def token_weights(list_lengths):
    slot_index = jnp.arange(SLOTS, dtype=jnp.int32)
    live_slots = slot_index[None, :] < list_lengths[:, None]
    scaled = jnp.where(
        live_slots, 1.0 / list_lengths[:, None].astype(jnp.float32), jnp.float32(0.0)
    )
    return scaled.reshape(-1)


def basis_routes(chips, splits):
    return [
        ((2 * k + b) * splits + s, (2 * s + b) * splits + (k - 3 * s) % splits)
        for k in range(chips)
        for b in range(2)
        for s in range(splits)
    ]


def body(tokens, out_grad, galore_basis, first_moment, second_moment, list_lengths):
    replicas = lax.axis_size("dp")
    splits = lax.axis_size("tensor")
    chips = replicas // 2
    core = lax.axis_index("dp") % 2
    parity = lax.axis_index("tensor") % 2
    rank = galore_basis.shape[1]
    half = rank // 2
    owned = rank // replicas
    columns = out_grad.shape[1]
    slots = tokens.shape[0]
    same_core = [[2 * i + c for i in range(chips)] for c in range(2)]
    same_parity = [[2 * i + p for i in range(splits // 2)] for p in range(2)]
    other_core = [(i, i ^ 1) for i in range(replicas)]
    neighbor = [(i, i ^ 1) for i in range(splits)]

    def coordinates_of(side):
        part = lax.dynamic_slice_in_dim(galore_basis, side * half, half, 1)
        return lax.dot_general(part, tokens, (((0,), (1,)), ((), ())), preferred_element_type=f32)

    received = lax.ppermute(coordinates_of(1 - parity).astype(bf16), "tensor", neighbor)
    block_rows = galore_basis.shape[0] * splits // replicas
    half_block = lax.dynamic_slice_in_dim(galore_basis, core * block_rows, block_rows, 0)
    local_basis = lax.ppermute(half_block, ("dp", "tensor"), basis_routes(chips, splits))
    kept = lax.optimization_barrier(coordinates_of(parity))
    pair_sum = (kept + received.astype(f32)).astype(bf16)
    arrived = exchange(pair_sum.reshape(splits // 2, rank // splits, slots), "tensor", same_parity)
    partner_grad = lax.ppermute(out_grad, "dp", other_core)
    both_grads = lax.optimization_barrier(jnp.concatenate([out_grad, partner_grad], axis=0))
    coordinates = arrived.astype(f32).sum(axis=0)
    weighted = (coordinates * token_weights(list_lengths)[None, :]).astype(bf16)
    by_core = weighted.reshape(2, owned, slots)
    own = lax.dynamic_index_in_dim(by_core, core, 0, keepdims=False)
    traded = lax.ppermute(lax.dynamic_index_in_dim(by_core, 1 - core, 0, keepdims=False), "dp", other_core)
    both = jnp.concatenate([own, traded], axis=1)
    near = copies_to_all(both, "tensor", splits // 2, same_parity).reshape(half // 2, 2 * slots)
    far = lax.ppermute(near, "tensor", neighbor)
    low = jnp.where(parity == 0, near, far)
    high = jnp.where(parity == 0, far, near)
    rows = jnp.concatenate([low, high], axis=0)
    chip_sum = jnp.dot(rows, both_grads, preferred_element_type=f32).astype(bf16)
    chip_sum = chip_sum.reshape(chips, owned, columns)
    gradient = exchange(chip_sum, "dp", same_core).astype(f32).sum(axis=0)

    new_first = beta_first * first_moment + (1.0 - beta_first) * gradient
    new_second = beta_second * second_moment + (1.0 - beta_second) * gradient * gradient
    corrected_first = new_first / (1.0 - beta_first**STEP)
    corrected_second = new_second / (1.0 - beta_second**STEP)
    update = (corrected_first / (jnp.sqrt(corrected_second) + epsilon)).astype(bf16)

    own_rows = copies_to_all(update, "dp", chips, same_core).reshape(half, columns)
    other_rows = lax.ppermute(own_rows, "dp", other_core)
    place = jnp.arange(rank, dtype=jnp.int32)
    within = place % half
    source = (within // owned) * (2 * owned) + jnp.where(place < half, core, 1 - core) * owned + within % owned
    pick = (place[:, None] == source[None, :]).astype(bf16)
    ordered = jnp.dot(local_basis, pick, preferred_element_type=f32).astype(bf16)
    expanded = jnp.dot(ordered[:, :half], own_rows, preferred_element_type=f32)
    expanded = expanded + jnp.dot(ordered[:, half:], other_rows, preferred_element_type=f32)
    weight_step = (-expanded).astype(bf16)
    return (new_first, new_second, weight_step)


def solution(mesh):
    in_specs = (
        P("dp", "tensor"),
        P("dp", "tensor"),
        P("tensor", None),
        P("dp", "tensor"),
        P("dp", "tensor"),
        P("dp"),
    )
    out_specs = (P("dp", "tensor"), P("dp", "tensor"), P("dp", "tensor"))
    return jax.shard_map(body, mesh=mesh, in_specs=in_specs, out_specs=out_specs, check_vma=False)
```

```python
import jax
import jax.numpy as jnp
from jax import lax
from jax.sharding import PartitionSpec as P


SLOTS = 128
STEP = 1000


beta_first = 0.9
beta_second = 0.999
epsilon = 1e-08

bf16 = jnp.bfloat16
f32 = jnp.float32


def exchange(tiles, axis, groups=None):
    return lax.all_to_all(tiles, axis, split_axis=0, concat_axis=0, tiled=True, axis_index_groups=groups)


def copies_to_all(x, axis, peers, groups=None):
    return exchange(jnp.broadcast_to(x, (peers, *x.shape)), axis, groups)


def token_weights(list_lengths):
    slot_index = jnp.arange(SLOTS, dtype=jnp.int32)
    live_slots = slot_index[None, :] < list_lengths[:, None]
    scaled = jnp.where(
        live_slots, 1.0 / list_lengths[:, None].astype(jnp.float32), jnp.float32(0.0)
    )
    return scaled.reshape(-1)


def reversed_bits(index, bits):
    return sum(((index >> i) & 1) << (bits - 1 - i) for i in range(bits))


def piece_routes(chips, splits):
    return [
        ((2 * k + b) * splits + s, (2 * s + b) * splits + (k - 3 * s) % splits)
        for k in range(chips)
        for b in range(2)
        for s in range(splits)
    ]


def body(tokens, out_grad, galore_basis, first_moment, second_moment, list_lengths):
    replicas = lax.axis_size("dp")
    splits = lax.axis_size("tensor")
    chips = replicas // 2
    core = lax.axis_index("dp") % 2
    parity = lax.axis_index("tensor") % 2
    rank = galore_basis.shape[1]
    half = rank // 2
    owned = rank // replicas
    columns = out_grad.shape[1]
    slots = tokens.shape[0]
    same_core = [[2 * i + c for i in range(chips)] for c in range(2)]
    same_parity = [[2 * i + p for i in range(splits // 2)] for p in range(2)]
    other_core = [(i, i ^ 1) for i in range(replicas)]
    neighbor = [(i, i ^ 1) for i in range(splits)]

    def coordinates_of(side):
        part = lax.dynamic_slice_in_dim(galore_basis, side * half, half, 1)
        return lax.dot_general(part, tokens, (((0,), (1,)), ((), ())), preferred_element_type=f32)

    received = lax.ppermute(coordinates_of(1 - parity).astype(bf16), "tensor", neighbor)
    split = lax.axis_index("tensor")
    levels = splits.bit_length() - 1
    block_rows = galore_basis.shape[0] * splits // replicas
    piece_rows = block_rows // splits
    served = (lax.axis_index("dp") // 2 - 3 * split) % splits
    start = core * block_rows + reversed_bits(served, levels) * piece_rows
    local_basis = lax.dynamic_slice_in_dim(galore_basis, start, piece_rows, 0)
    local_basis = lax.ppermute(local_basis, ("dp", "tensor"), piece_routes(chips, splits))
    for level in reversed(range(levels)):
        distance = 1 << level
        theirs = lax.ppermute(local_basis, "tensor", [(i, i ^ distance) for i in range(splits)])
        first = (split >> level) % 2 == 0
        halves = (jnp.where(first, local_basis, theirs), jnp.where(first, theirs, local_basis))
        local_basis = jnp.concatenate(halves, axis=0)
    kept = lax.optimization_barrier(coordinates_of(parity))
    pair_sum = (kept + received.astype(f32)).astype(bf16)
    arrived = exchange(pair_sum.reshape(splits // 2, rank // splits, slots), "tensor", same_parity)
    partner_grad = lax.ppermute(out_grad, "dp", other_core)
    coordinates = arrived.astype(f32).sum(axis=0)
    weighted = (coordinates * token_weights(list_lengths)[None, :]).astype(bf16)
    by_core = weighted.reshape(2, owned, slots)
    own = lax.dynamic_index_in_dim(by_core, core, 0, keepdims=False)
    traded = lax.ppermute(lax.dynamic_index_in_dim(by_core, 1 - core, 0, keepdims=False), "dp", other_core)
    both = jnp.concatenate([own, traded], axis=1)
    near = copies_to_all(both, "tensor", splits // 2, same_parity).reshape(half // 2, 2 * slots)
    far = lax.ppermute(near, "tensor", neighbor)
    low = jnp.where(parity == 0, near, far)
    high = jnp.where(parity == 0, far, near)
    rows = jnp.concatenate([low, high], axis=0)
    kept = jnp.dot(rows[:, :slots], out_grad, preferred_element_type=f32)
    kept = kept + jnp.dot(rows[:, slots:], partner_grad, preferred_element_type=f32)
    chip_sum = kept.astype(bf16).reshape(chips, owned, columns)
    gradient = exchange(chip_sum, "dp", same_core).astype(f32).sum(axis=0)

    new_first = beta_first * first_moment + (1.0 - beta_first) * gradient
    new_second = beta_second * second_moment + (1.0 - beta_second) * gradient * gradient
    corrected_first = new_first / (1.0 - beta_first**STEP)
    corrected_second = new_second / (1.0 - beta_second**STEP)
    update = (corrected_first / (jnp.sqrt(corrected_second) + epsilon)).astype(bf16)

    own_rows = copies_to_all(update, "dp", chips, same_core).reshape(half, columns)
    other_rows = lax.ppermute(own_rows, "dp", other_core)
    place = jnp.arange(rank, dtype=jnp.int32)
    within = place % half
    source = (within // owned) * (2 * owned) + jnp.where(place < half, core, 1 - core) * owned + within % owned
    pick = (place[:, None] == source[None, :]).astype(bf16)
    ordered = jnp.dot(local_basis, pick, preferred_element_type=f32).astype(bf16)
    expanded = jnp.dot(ordered[:, :half], own_rows, preferred_element_type=f32)
    expanded = expanded + jnp.dot(ordered[:, half:], other_rows, preferred_element_type=f32)
    weight_step = (-expanded).astype(bf16)
    return (new_first, new_second, weight_step)


def solution(mesh):
    in_specs = (
        P("dp", "tensor"),
        P("dp", "tensor"),
        P("tensor", None),
        P("dp", "tensor"),
        P("dp", "tensor"),
        P("dp"),
    )
    out_specs = (P("dp", "tensor"), P("dp", "tensor"), P("dp", "tensor"))
    return jax.shard_map(body, mesh=mesh, in_specs=in_specs, out_specs=out_specs, check_vma=False)
```

```python
import jax
import jax.numpy as jnp
from jax import lax
from jax.sharding import PartitionSpec as P


SLOTS = 128
STEP = 1000


beta_first = 0.9
beta_second = 0.999
epsilon = 1e-08

bf16 = jnp.bfloat16
f32 = jnp.float32


def exchange(tiles, axis, groups=None):
    return lax.all_to_all(tiles, axis, split_axis=0, concat_axis=0, tiled=True, axis_index_groups=groups)


def copies_to_all(x, axis, peers, groups=None):
    return exchange(jnp.broadcast_to(x, (peers, *x.shape)), axis, groups)


def token_weights(list_lengths):
    slot_index = jnp.arange(SLOTS, dtype=jnp.int32)
    live_slots = slot_index[None, :] < list_lengths[:, None]
    scaled = jnp.where(
        live_slots, 1.0 / list_lengths[:, None].astype(jnp.float32), jnp.float32(0.0)
    )
    return scaled.reshape(-1)


def basis_routes(chips, splits):
    return [
        ((2 * k + b) * splits + s, (2 * s + b) * splits + (k - 3 * s) % splits)
        for k in range(chips)
        for b in range(2)
        for s in range(splits)
    ]


def body(tokens, out_grad, galore_basis, first_moment, second_moment, list_lengths):
    replicas = lax.axis_size("dp")
    splits = lax.axis_size("tensor")
    chips = replicas // 2
    core = lax.axis_index("dp") % 2
    parity = lax.axis_index("tensor") % 2
    rank = galore_basis.shape[1]
    half = rank // 2
    owned = rank // replicas
    columns = out_grad.shape[1]
    slots = tokens.shape[0]
    same_core = [[2 * i + c for i in range(chips)] for c in range(2)]
    same_parity = [[2 * i + p for i in range(splits // 2)] for p in range(2)]
    other_core = [(i, i ^ 1) for i in range(replicas)]
    neighbor = [(i, i ^ 1) for i in range(splits)]

    def coordinates_of(side):
        part = lax.dynamic_slice_in_dim(galore_basis, side * half, half, 1)
        return lax.dot_general(part, tokens, (((0,), (1,)), ((), ())), preferred_element_type=f32)

    received = lax.ppermute(coordinates_of(1 - parity).astype(bf16), "tensor", neighbor)
    block_rows = galore_basis.shape[0] * splits // replicas
    half_block = lax.dynamic_slice_in_dim(galore_basis, core * block_rows, block_rows, 0)
    local_basis = lax.ppermute(half_block, ("dp", "tensor"), basis_routes(chips, splits))
    kept = lax.optimization_barrier(coordinates_of(parity))
    pair_sum = (kept + received.astype(f32)).astype(bf16)
    arrived = exchange(pair_sum.reshape(splits // 2, rank // splits, slots), "tensor", same_parity)
    partner_grad = lax.ppermute(out_grad, "dp", other_core)
    coordinates = arrived.astype(f32).sum(axis=0)
    weighted = (coordinates * token_weights(list_lengths)[None, :]).astype(bf16)
    by_core = weighted.reshape(2, owned, slots)
    own = lax.dynamic_index_in_dim(by_core, core, 0, keepdims=False)
    traded = lax.ppermute(lax.dynamic_index_in_dim(by_core, 1 - core, 0, keepdims=False), "dp", other_core)
    both = jnp.concatenate([own, traded], axis=1)
    near = copies_to_all(both, "tensor", splits // 2, same_parity).reshape(half // 2, 2 * slots)
    far = lax.ppermute(near, "tensor", neighbor)
    low = jnp.where(parity == 0, near, far)
    high = jnp.where(parity == 0, far, near)
    rows = jnp.concatenate([low, high], axis=0)
    kept = jnp.dot(rows[:, :slots], out_grad, preferred_element_type=f32)
    kept = kept + jnp.dot(rows[:, slots:], partner_grad, preferred_element_type=f32)
    chip_sum = kept.astype(bf16).reshape(chips, owned, columns)
    gradient = exchange(chip_sum, "dp", same_core).astype(f32).sum(axis=0)

    new_first = beta_first * first_moment + (1.0 - beta_first) * gradient
    new_second = beta_second * second_moment + (1.0 - beta_second) * gradient * gradient
    corrected_first = new_first / (1.0 - beta_first**STEP)
    corrected_second = new_second / (1.0 - beta_second**STEP)
    update = (corrected_first / (jnp.sqrt(corrected_second) + epsilon)).astype(bf16)

    own_rows = copies_to_all(update, "dp", chips, same_core).reshape(half, columns)
    other_rows = lax.ppermute(own_rows, "dp", other_core)
    place = jnp.arange(rank, dtype=jnp.int32)
    within = place % half
    source = (within // owned) * (2 * owned) + jnp.where(place < half, core, 1 - core) * owned + within % owned
    pick = (place[:, None] == source[None, :]).astype(bf16)
    ordered = jnp.dot(local_basis, pick, preferred_element_type=f32).astype(bf16)
    expanded = jnp.dot(ordered[:, :half], own_rows, preferred_element_type=f32)
    expanded = expanded + jnp.dot(ordered[:, half:], other_rows, preferred_element_type=f32)
    weight_step = (-expanded).astype(bf16)
    return (new_first, new_second, weight_step)


def solution(mesh):
    in_specs = (
        P("dp", "tensor"),
        P("dp", "tensor"),
        P("tensor", None),
        P("dp", "tensor"),
        P("dp", "tensor"),
        P("dp"),
    )
    out_specs = (P("dp", "tensor"), P("dp", "tensor"), P("dp", "tensor"))
    return jax.shard_map(body, mesh=mesh, in_specs=in_specs, out_specs=out_specs, check_vma=False)
```

```python
import jax
import jax.numpy as jnp
from jax import lax
from jax.sharding import PartitionSpec as P


SLOTS = 128
STEP = 1000


beta_first = 0.9
beta_second = 0.999
epsilon = 1e-08

bf16 = jnp.bfloat16
f32 = jnp.float32


def exchange(tiles, axis, groups=None):
    return lax.all_to_all(tiles, axis, split_axis=0, concat_axis=0, tiled=True, axis_index_groups=groups)


def copies_to_all(x, axis, peers, groups=None):
    return exchange(jnp.broadcast_to(x, (peers, *x.shape)), axis, groups)


def token_weights(list_lengths):
    slot_index = jnp.arange(SLOTS, dtype=jnp.int32)
    live_slots = slot_index[None, :] < list_lengths[:, None]
    scaled = jnp.where(
        live_slots, 1.0 / list_lengths[:, None].astype(jnp.float32), jnp.float32(0.0)
    )
    return scaled.reshape(-1)


def basis_routes(chips, splits):
    return [
        ((2 * k + b) * splits + s, (2 * s + b) * splits + (k - s) % splits)
        for k in range(chips)
        for b in range(2)
        for s in range(splits)
    ]


def body(tokens, out_grad, galore_basis, first_moment, second_moment, list_lengths):
    replicas = lax.axis_size("dp")
    splits = lax.axis_size("tensor")
    chips = replicas // 2
    core = lax.axis_index("dp") % 2
    parity = lax.axis_index("tensor") % 2
    rank = galore_basis.shape[1]
    half = rank // 2
    owned = rank // replicas
    columns = out_grad.shape[1]
    slots = tokens.shape[0]
    chip_order = [(i % 2) * (chips // 2) + i // 2 for i in range(chips)]
    same_core = [[2 * chip + c for chip in chip_order] for c in range(2)]
    same_parity = [[2 * i + p for i in range(splits // 2)] for p in range(2)]
    other_core = [(i, i ^ 1) for i in range(replicas)]
    neighbor = [(i, i ^ 1) for i in range(splits)]

    def coordinates_of(side):
        part = lax.dynamic_slice_in_dim(galore_basis, side * half, half, 1)
        return lax.dot_general(part, tokens, (((0,), (1,)), ((), ())), preferred_element_type=f32)

    received = lax.ppermute(coordinates_of(1 - parity).astype(bf16), "tensor", neighbor)
    block_rows = galore_basis.shape[0] * splits // replicas
    half_block = lax.dynamic_slice_in_dim(galore_basis, core * block_rows, block_rows, 0)
    local_basis = lax.ppermute(half_block, ("dp", "tensor"), basis_routes(chips, splits))
    kept = lax.optimization_barrier(coordinates_of(parity))
    pair_sum = (kept + received.astype(f32)).astype(bf16)
    arrived = exchange(pair_sum.reshape(splits // 2, rank // splits, slots), "tensor", same_parity)
    partner_grad = lax.ppermute(out_grad, "dp", other_core)
    coordinates = arrived.astype(f32).sum(axis=0)
    weighted = (coordinates * token_weights(list_lengths)[None, :]).astype(bf16)
    by_core = weighted.reshape(2, owned, slots)
    own = lax.dynamic_index_in_dim(by_core, core, 0, keepdims=False)
    traded = lax.ppermute(lax.dynamic_index_in_dim(by_core, 1 - core, 0, keepdims=False), "dp", other_core)
    both = jnp.concatenate([own, traded], axis=1)
    rows = lax.all_gather(both, "tensor", axis=0, tiled=True)
    kept = jnp.dot(rows[:, :slots], out_grad, preferred_element_type=f32)
    kept = kept + jnp.dot(rows[:, slots:], partner_grad, preferred_element_type=f32)
    chip_sum = kept.astype(bf16).reshape(chips, owned, columns)
    gradient = exchange(chip_sum, "dp", same_core).astype(f32).sum(axis=0)

    new_first = beta_first * first_moment + (1.0 - beta_first) * gradient
    new_second = beta_second * second_moment + (1.0 - beta_second) * gradient * gradient
    corrected_first = new_first / (1.0 - beta_first**STEP)
    corrected_second = new_second / (1.0 - beta_second**STEP)
    update = (corrected_first / (jnp.sqrt(corrected_second) + epsilon)).astype(bf16)

    own_rows = copies_to_all(update, "dp", chips, same_core).reshape(half, columns)
    other_rows = lax.ppermute(own_rows, "dp", other_core)
    place = jnp.arange(rank, dtype=jnp.int32)
    within = place % half
    chip = within // owned
    chip = chip % 2 * (chips // 2) + chip // 2
    source = chip * (2 * owned) + jnp.where(place < half, core, 1 - core) * owned + within % owned
    pick = (place[:, None] == source[None, :]).astype(bf16)
    ordered = jnp.dot(local_basis, pick, preferred_element_type=f32).astype(bf16)
    expanded = jnp.dot(ordered[:, :half], own_rows, preferred_element_type=f32)
    expanded = expanded + jnp.dot(ordered[:, half:], other_rows, preferred_element_type=f32)
    weight_step = (-expanded).astype(bf16)
    return (new_first, new_second, weight_step)


def solution(mesh):
    in_specs = (
        P("dp", "tensor"),
        P("dp", "tensor"),
        P("tensor", None),
        P("dp", "tensor"),
        P("dp", "tensor"),
        P("dp"),
    )
    out_specs = (P("dp", "tensor"), P("dp", "tensor"), P("dp", "tensor"))
    return jax.shard_map(body, mesh=mesh, in_specs=in_specs, out_specs=out_specs, check_vma=False)
```
